8 devices in a mesh: dp: 1 (over z), tp: 8 (over y, x, core).
Axes of the slice: x: 2, y: 2, z: 1, core: 2. Of those that a mesh axis runs over, the one named last changes fastest.
Arguments:
- hidden: bfloat16 [2, 2048, 2048], P('dp')
- attn_mask: int32 [2, 2048], P('dp')
- ln1_gain: bfloat16 [2, 2048], replicated
- ln1_bias: bfloat16 [2, 2048], replicated
- w_query: bfloat16 [2, 2048, 32, 64], P(None, None, 'tp')
- b_query: bfloat16 [2, 32, 64], P(None, 'tp')
- w_key: bfloat16 [2, 2048, 32, 64], P(None, None, 'tp')
- b_key: bfloat16 [2, 32, 64], P(None, 'tp')
- w_value: bfloat16 [2, 2048, 32, 64], P(None, None, 'tp')
- b_value: bfloat16 [2, 32, 64], P(None, 'tp')
- w_out: bfloat16 [2, 32, 64, 2048], P(None, 'tp')
- b_out: bfloat16 [2, 2048], replicated
- ln2_gain: bfloat16 [2, 2048], replicated
- ln2_bias: bfloat16 [2, 2048], replicated
- w_fc1: bfloat16 [2, 2048, 8192], P(None, None, 'tp')
- b_fc1: bfloat16 [2, 8192], P(None, 'tp')
- w_fc2: bfloat16 [2, 8192, 2048], P(None, 'tp')
- b_fc2: bfloat16 [2, 2048], replicated
Outputs:
- output 1: bfloat16 [2, 2048, 2048], P('dp')
- output 2: bfloat16 [2, 2, 32, 4096, 64], P(None, 'dp', 'tp')
- output 3: bfloat16 [2, 2, 32, 4096, 64], P(None, 'dp', 'tp')
All inputs are finite; a program needn't handle non-finite values.
Results may differ from the reference program's by a relative error of at most 0.0151403.
Values are sent between devices in bfloat16 or wider.
A program may use at most 1 GiB of HBM per device.

```python
import jax
import jax.numpy as jnp
from jax import lax

LAYERS = 2
PROMPTS = 2
SEQ_LEN = 2048
CACHE_LEN = 4096
D_MODEL = 2048
HEADS = 32
HEAD_DIM = 64
FF_DIM = 8192


def setup_inputs(seed: int = 0, part: int = 0) -> dict:
    part_key = jax.random.fold_in(jax.random.key(seed), part)
    key_hidden, key_pad, key_row = jax.random.split(part_key, 3)
    shared = jax.random.split(jax.random.key(seed + 1), 16)
    hidden = jax.random.normal(key_hidden, (PROMPTS, SEQ_LEN, D_MODEL), jnp.float32).astype(jnp.bfloat16)
    half_len = SEQ_LEN // 2
    pad_len = jax.random.randint(key_pad, (PROMPTS,), 0, half_len + 1)
    longest = jax.random.randint(key_row, (), 0, PROMPTS)
    pad_len = jnp.where(jnp.arange(PROMPTS) == longest, half_len, pad_len)
    attn_mask = (jnp.arange(SEQ_LEN)[None, :] >= pad_len[:, None]).astype(jnp.int32)

    def draw(index, shape, scale, offset):
        return (offset + scale * jax.random.normal(shared[index], shape, jnp.float32)).astype(jnp.bfloat16)

    d_scale = D_MODEL ** -0.5
    head_shape = (LAYERS, D_MODEL, HEADS, HEAD_DIM)
    bias_shape = (LAYERS, HEADS, HEAD_DIM)
    return {
        'hidden': hidden,
        'attn_mask': attn_mask,
        'ln1_gain': draw(0, (LAYERS, D_MODEL), 0.2, 1.0),
        'ln1_bias': draw(1, (LAYERS, D_MODEL), 0.2, 0.0),
        'w_query': draw(2, head_shape, d_scale, 0.0),
        'b_query': draw(3, bias_shape, 1.5, 0.0),
        'w_key': draw(4, head_shape, d_scale, 0.0),
        'b_key': draw(5, bias_shape, 0.5, 0.0),
        'w_value': draw(6, head_shape, d_scale, 0.0),
        'b_value': draw(7, bias_shape, 0.5, 0.0),
        'w_out': draw(8, (LAYERS, HEADS, HEAD_DIM, D_MODEL), d_scale, 0.0),
        'b_out': draw(9, (LAYERS, D_MODEL), 0.5, 0.0),
        'ln2_gain': draw(10, (LAYERS, D_MODEL), 0.2, 1.0),
        'ln2_bias': draw(11, (LAYERS, D_MODEL), 0.2, 0.0),
        'w_fc1': draw(12, (LAYERS, D_MODEL, FF_DIM), d_scale, 0.0),
        'b_fc1': draw(13, (LAYERS, FF_DIM), 0.5, 0.0),
        'w_fc2': draw(14, (LAYERS, FF_DIM, D_MODEL), FF_DIM ** -0.5, 0.0),
        'b_fc2': draw(15, (LAYERS, D_MODEL), 0.5, 0.0),
    }


def layer_norm(values, gain, shift):
    as_float = values.astype(jnp.float32)
    center = as_float - jnp.mean(as_float, axis=-1, keepdims=True)
    variance = jnp.mean(center * center, axis=-1, keepdims=True)
    normed = center * lax.rsqrt(variance + 1e-5)
    return (normed * gain.astype(jnp.float32) + shift.astype(jnp.float32)).astype(jnp.bfloat16)


def attend_one(operands):
    query_h, key_h, value_h, key_ok = operands
    scores = jnp.dot(query_h, key_h.T, preferred_element_type=jnp.float32)
    positions = jnp.arange(SEQ_LEN)
    allowed = (positions[None, :] <= positions[:, None]) & key_ok[None, :]
    row_max = jnp.max(jnp.where(allowed, scores, -1e30), axis=-1, keepdims=True)
    exp_scores = jnp.exp(jnp.where(allowed, scores - row_max, -jnp.inf))
    row_sum = jnp.sum(exp_scores, axis=-1, keepdims=True)
    context = jnp.dot(exp_scores.astype(jnp.bfloat16), value_h, preferred_element_type=jnp.float32)
    return (context / jnp.maximum(row_sum, 1.0)).astype(jnp.bfloat16)


def reference(hidden, attn_mask, ln1_gain, ln1_bias, w_query, b_query, w_key, b_key, w_value, b_value, w_out, b_out, ln2_gain, ln2_bias, w_fc1, b_fc1, w_fc2, b_fc2):
    scale = HEAD_DIM ** -0.5
    key_ok = jnp.repeat(attn_mask > 0, HEADS, axis=0)
    rows = PROMPTS * SEQ_LEN
    flat_shape = (PROMPTS * HEADS, SEQ_LEN, HEAD_DIM)
    cache_pad = ((0, 0), (0, 0), (0, CACHE_LEN - SEQ_LEN), (0, 0))

    def project(normed, weight, bias):
        flat = jnp.dot(normed.reshape(rows, D_MODEL), weight.reshape(D_MODEL, HEADS * HEAD_DIM), preferred_element_type=jnp.float32)
        heads = flat.reshape(PROMPTS, SEQ_LEN, HEADS, HEAD_DIM) + bias.astype(jnp.float32)
        return jnp.transpose(heads, (0, 2, 1, 3))

    def layer_step(residual, weights):
        (norm1_gain, norm1_bias, query_w, query_b, key_w, key_b, value_w, value_b, out_w, out_b,
         norm2_gain, norm2_bias, fc1_w, fc1_b, fc2_w, fc2_b) = weights
        normed = layer_norm(residual, norm1_gain, norm1_bias)
        query = (project(normed, query_w, query_b) * scale).astype(jnp.bfloat16)
        key_heads = project(normed, key_w, key_b).astype(jnp.bfloat16)
        value_heads = project(normed, value_w, value_b).astype(jnp.bfloat16)
        context = lax.map(attend_one, (query.reshape(flat_shape), key_heads.reshape(flat_shape), value_heads.reshape(flat_shape), key_ok))
        context = jnp.transpose(context.reshape(PROMPTS, HEADS, SEQ_LEN, HEAD_DIM), (0, 2, 1, 3)).reshape(rows, D_MODEL)
        attn_out = jnp.dot(context, out_w.reshape(D_MODEL, D_MODEL), preferred_element_type=jnp.float32)
        residual = (residual.astype(jnp.float32) + attn_out.reshape(PROMPTS, SEQ_LEN, D_MODEL) + out_b.astype(jnp.float32)).astype(jnp.bfloat16)
        normed = layer_norm(residual, norm2_gain, norm2_bias)
        inner = jnp.dot(normed.reshape(rows, D_MODEL), fc1_w, preferred_element_type=jnp.float32) + fc1_b.astype(jnp.float32)
        inner = jnp.maximum(inner, 0.0).astype(jnp.bfloat16)
        mlp_out = jnp.dot(inner, fc2_w, preferred_element_type=jnp.float32).reshape(PROMPTS, SEQ_LEN, D_MODEL)
        residual = (residual.astype(jnp.float32) + mlp_out + fc2_b.astype(jnp.float32)).astype(jnp.bfloat16)
        return residual, (jnp.pad(key_heads, cache_pad), jnp.pad(value_heads, cache_pad))

    weights = (ln1_gain, ln1_bias, w_query, b_query, w_key, b_key, w_value, b_value, w_out, b_out,
               ln2_gain, ln2_bias, w_fc1, b_fc1, w_fc2, b_fc2)
    out_hidden, caches = lax.scan(layer_step, hidden, weights)
    return out_hidden, caches[0], caches[1]
```

```python
import functools

import jax
import jax.numpy as jnp
from jax import lax
from jax.experimental import pallas as pl
from jax.experimental.pallas import tpu as pltpu
from jax.sharding import PartitionSpec as P

LN_EPS = 1e-5
NT = (((1,), (1,)), ((), ()))
BLK = 256
F32 = jnp.float32
BF16 = jnp.bfloat16


FLIP_C = [(i, i ^ 1) for i in range(8)]
FLIP_F = [(i, i ^ (2 if i & 1 else 4)) for i in range(8)]
FLIP_S = [(i, i ^ (4 if i & 1 else 2)) for i in range(8)]


def norm_rows(x, gain, shift):
    center = x - jnp.mean(x, axis=-1, keepdims=True)
    variance = jnp.mean(center * center, axis=-1, keepdims=True)
    normed = center * lax.rsqrt(variance + LN_EPS)
    return (normed * gain + shift).astype(BF16)


def const_spec(shape, index):
    return pl.BlockSpec(shape, lambda *_: index, pipeline_mode=pl.Buffered(1))


def qkv_kernel(scale, which_ref, *refs):
    x_ref, g_ref, s_ref, wq_ref, wk_ref, wv_ref, bq_ref, bk_ref, bv_ref = refs[:9]
    q_ref, k_ref, v_ref, kc_ref, vc_ref = refs[-5:]
    h = norm_rows(x_ref[...].astype(F32), g_ref[...], s_ref[...])
    q = lax.dot_general(h, wq_ref[0], NT, preferred_element_type=F32)
    q_ref[...] = ((q + bq_ref[...]) * scale).astype(BF16)
    k = (lax.dot_general(wk_ref[0], h, NT, preferred_element_type=F32) + bk_ref[...]).astype(BF16)
    v = (lax.dot_general(wv_ref[0], h, NT, preferred_element_type=F32) + bv_ref[...]).astype(BF16)
    k_ref[...] = k
    v_ref[...] = v
    kc_ref[0, 0] = k
    vc_ref[0, 0] = v


def qkv(which, half, caches, cache_shape, x, gain, shift, wq, wk, wv, bq, bk, bv, layer, scale):
    rows, d = x.shape
    n = wq.shape[1]
    blocks = rows // BLK
    w_spec = const_spec((1, n, d), (layer, 0, 0))
    in_specs = [pl.BlockSpec((BLK, d), lambda i, w: (i, 0)), const_spec((1, d), (0, 0)), const_spec((1, d), (0, 0)),
                w_spec, w_spec, w_spec, const_spec((1, n), (0, 0)), const_spec((n, 1), (0, 0)), const_spec((n, 1), (0, 0))]
    args = [x, gain, shift, wq, wk, wv, bq, bk, bv]
    aliases = {}
    if caches is not None:
        in_specs += [pl.BlockSpec(memory_space=pl.ANY)] * 2
        args += list(caches)
        aliases = {10: 3, 11: 4}
    cache_spec = pl.BlockSpec((1, 1, n, BLK), lambda i, w: (layer, w[0], 0, half * blocks + i))
    return pl.pallas_call(
        functools.partial(qkv_kernel, scale),
        grid_spec=pltpu.PrefetchScalarGridSpec(
            num_scalar_prefetch=1,
            grid=(blocks,),
            in_specs=in_specs,
            out_specs=[pl.BlockSpec((BLK, n), lambda i, w: (i, 0))] + [pl.BlockSpec((n, BLK), lambda i, w: (0, i))] * 2 + [cache_spec] * 2,
        ),
        out_shape=[jax.ShapeDtypeStruct((rows, n), BF16)] + [jax.ShapeDtypeStruct((n, rows), BF16)] * 2 + [jax.ShapeDtypeStruct(cache_shape, BF16)] * 2,
        input_output_aliases=aliases,
        cost_estimate=pl.CostEstimate(flops=2 * rows * d * 3 * n, bytes_accessed=rows * d * 2 + 3 * n * d * 2, transcendentals=0),
        name="ln_qkv",
    )(which, *args)


def tail_kernel(kin, vin, kc_ref, vc_ref):
    kc_ref[...] = jnp.zeros_like(kc_ref)
    vc_ref[...] = jnp.zeros_like(vc_ref)


def zero_tail(caches):
    layers, prompts, n, length = caches[0].shape
    spec = pl.BlockSpec((1, 1, n, length // 2), lambda i, j: (i, j, 0, 1))
    return pl.pallas_call(
        tail_kernel,
        grid=(layers, prompts),
        in_specs=[pl.BlockSpec(memory_space=pl.ANY)] * 2,
        out_specs=[spec, spec],
        out_shape=[jax.ShapeDtypeStruct(v.shape, v.dtype) for v in caches],
        input_output_aliases={0: 0, 1: 1},
        name="zero_tail",
    )(*caches)


def attn_kernel(num_old, head_dim, *refs):
    prefix_ref, q_ref = refs[:2]
    k_refs = refs[2:2 + num_old + 1]
    v_refs = refs[2 + num_old + 1:4 + 2 * num_old]
    c_ref = refs[-1]
    head = pl.program_id(0)
    rows, n = q_ref.shape
    lane = lax.broadcasted_iota(jnp.int32, (1, n), 1)
    mine = lane // head_dim == head
    prefix = prefix_ref[0]
    diag = lax.broadcasted_iota(jnp.int32, (BLK, BLK), 1) <= lax.broadcasted_iota(jnp.int32, (BLK, BLK), 0)
    for i in range(rows // BLK):
        q = jnp.where(mine, q_ref[pl.ds(i * BLK, BLK), :], 0)
        pieces = []
        base = 0
        for k_ref, v_ref in zip(k_refs, v_refs):
            last = base == num_old * rows
            size = (i + 1) * BLK if last else rows
            for lo in range(0, size, BLK):
                width = BLK
                s = jnp.dot(q, k_ref[:, pl.ds(lo, width)], preferred_element_type=F32)
                if base == 0:
                    key = lax.broadcasted_iota(jnp.int32, (1, width), 1) + lo
                    s = s + jnp.where(key >= prefix, 0.0, -jnp.inf)
                if last and lo == i * BLK:
                    s = jnp.where(diag, s, -jnp.inf)
                pieces.append((s, v_ref, lo))
            base += rows
        top = pieces[0][0]
        for s, _, _ in pieces[1:]:
            top = jnp.maximum(top, s)
        row_max = jnp.maximum(jnp.max(top, axis=-1, keepdims=True), -1e30)
        total = None
        ctx = None
        for s, v_ref, lo in pieces:
            p = jnp.exp(s - row_max)
            total = p if total is None else total + p
            part = lax.dot_general(p.astype(BF16), v_ref[:, pl.ds(lo, BLK)], NT, preferred_element_type=F32)
            ctx = part if ctx is None else ctx + part
        row_sum = jnp.sum(total, axis=-1, keepdims=True)
        out = (ctx / jnp.maximum(row_sum, 1.0)).astype(BF16)
        here = pl.ds(i * BLK, BLK)
        c_ref[here, :] = jnp.where(mine, out, c_ref[here, :])


def attend(prefix, q, ks, vs, heads):
    rows, n = q.shape
    num_old = len(ks) - 1
    whole = [const_spec(q.shape, (0, 0))] + [const_spec(k.shape, (0, 0)) for k in ks] * 2
    area = rows * rows * num_old + rows * rows // 2
    return pl.pallas_call(
        functools.partial(attn_kernel, num_old, n // heads),
        grid=(heads,),
        in_specs=[pl.BlockSpec(memory_space=pltpu.SMEM)] + whole,
        out_specs=pl.BlockSpec((rows, n), lambda i: (0, 0)),
        out_shape=jax.ShapeDtypeStruct((rows, n), BF16),
        cost_estimate=pl.CostEstimate(flops=area * heads * n * 4, bytes_accessed=rows * n * 8, transcendentals=area * heads),
        name="attend",
    )(prefix, q, *ks, *vs)


def mlp_kernel(with_attn, order_ref, *refs):
    if with_attn:
        c_lo, c_hi, w_lo, w_hi = refs[:4]
        refs = refs[4:]
    x_ref, bo_ref, g_ref, s_ref, b1_ref, w1_ref, w2_ref, send_ref, keep_ref, mid_ref = refs[:10]
    i = pl.program_id(0)
    half = pl.num_programs(0) // 2
    x = x_ref[...].astype(F32)
    if with_attn:
        c_all = refs[10]
        for j in range(4):
            c_all[0, :, j * 256:(j + 1) * 256] = c_lo[j]
            c_all[1, :, j * 256:(j + 1) * 256] = c_hi[j]
        attn = jnp.dot(c_all[0], w_lo[...], preferred_element_type=F32) + jnp.dot(c_all[1], w_hi[...], preferred_element_type=F32)
        x = x + attn
    mid = (x + bo_ref[...]).astype(BF16)
    mid_ref[...] = mid
    g = norm_rows(mid.astype(F32), g_ref[...], s_ref[...])
    u = jnp.dot(g, w1_ref[0], preferred_element_type=F32) + b1_ref[...]
    u = jnp.maximum(u, 0.0).astype(BF16)
    part = jnp.dot(u, w2_ref[0], preferred_element_type=F32).astype(BF16)

    @pl.when(i < half)
    def _():
        send_ref[...] = part

    @pl.when(i >= half)
    def _():
        keep_ref[...] = part


def mlp(core, ctx, w_out, x, b_out, gain, shift, b1, w1, w2, layer):
    rows, d = x.shape
    f = w1.shape[2]
    n = rows // BLK
    half = n // 2
    order = (1 - core) * half
    order = jnp.stack([order]).astype(jnp.int32)
    row_of = lambda i, o: lax.rem(i + o[0], n)
    in_specs, args, scratch = [], [], []
    if ctx is not None:
        in_specs += [pl.BlockSpec((4, BLK, 256), lambda i, o: (0, row_of(i, o), 0))] * 2
        in_specs += [const_spec((d // 2, d), (0, 0))] * 2
        args += [*ctx, *w_out]
        scratch = [pltpu.VMEM((2, BLK, d // 2), BF16)]
    in_specs += [pl.BlockSpec((BLK, d), lambda i, o: (row_of(i, o), 0))] + [const_spec((1, d), (0, 0))] * 3
    in_specs += [const_spec((1, f), (0, 0)), const_spec((1, d, f), (layer, 0, 0)), const_spec((1, f, d), (layer, 0, 0))]
    args += [x, b_out, gain, shift, b1, w1, w2]
    flops = 4 * rows * d * f + (2 * rows * d * d if ctx is not None else 0)
    return pl.pallas_call(
        functools.partial(mlp_kernel, ctx is not None),
        grid_spec=pltpu.PrefetchScalarGridSpec(
            num_scalar_prefetch=1,
            grid=(n,),
            in_specs=in_specs,
            out_specs=[pl.BlockSpec((BLK, d), lambda i, o: (jnp.minimum(i, half - 1), 0)),
                       pl.BlockSpec((BLK, d), lambda i, o: (jnp.maximum(i - half, 0), 0)),
                       pl.BlockSpec((BLK, d), lambda i, o: (row_of(i, o), 0))],
            scratch_shapes=scratch,
        ),
        out_shape=[jax.ShapeDtypeStruct((rows // 2, d), BF16), jax.ShapeDtypeStruct((rows // 2, d), BF16), jax.ShapeDtypeStruct((rows, d), BF16)],
        compiler_params=pltpu.CompilerParams(vmem_limit_bytes=56 * 1024 * 1024),
        cost_estimate=pl.CostEstimate(flops=flops, bytes_accessed=rows * d * 8 + 4 * d * f, transcendentals=0),
        name="proj_mlp" if ctx is not None else "mlp",
    )(order, *args)


def solution(mesh):
    rep_vec = P(None, None)
    head_w = P(None, None, 'tp', None)
    head_b = P(None, 'tp', None)
    out_w = P(None, 'tp', None, None)
    in_specs = (P('dp', None, None), P('dp', None), rep_vec, rep_vec, head_w, head_b, head_w, head_b, head_w, head_b,
                out_w, rep_vec, rep_vec, rep_vec, P(None, None, 'tp'), P(None, 'tp'), P(None, 'tp', None), rep_vec)
    cache_spec = P(None, 'dp', 'tp', None, None)
    out_specs = (P('dp', None, None), cache_spec, cache_spec)

    def local_run(hidden, attn_mask, ln1_gain, ln1_bias, w_query, b_query, w_key, b_key, w_value, b_value, w_out, b_out, ln2_gain, ln2_bias, w_fc1, b_fc1, w_fc2, b_fc2):
        prompts, seq_len, d = hidden.shape
        num_layers, _, heads, head_dim = w_query.shape
        n = heads * head_dim
        rows = seq_len // 2
        scale = head_dim ** -0.5
        me = lax.axis_index('tp')
        core = me % 2
        bit_x, bit_y = (me // 2) % 2, me // 4
        first = jnp.where(core == 0, bit_y, bit_x)
        second = jnp.where(core == 0, bit_x, bit_y)

        prefix = jnp.sum((attn_mask == 0).astype(jnp.int32), axis=1)
        swap = prefix[1] == rows
        pre_a = jnp.where(swap, prefix[1], prefix[0])
        pre_b = jnp.where(swap, prefix[0], prefix[1])
        zero = jnp.zeros((1,), jnp.int32)
        pre_b1 = jnp.stack([pre_b])
        a_id = jnp.where(swap, 1, 0)

        def take(which, half):
            return lax.dynamic_slice(hidden, (which, half * rows, 0), (1, rows, d))[0]

        xs = {'P': take(a_id, 0), 'A': take(a_id, 1), 'B': take(1 - a_id, 0), 'C': take(1 - a_id, 1)}

        def head_weights(w):
            return jnp.transpose(w, (0, 2, 3, 1)).reshape(num_layers, n, d)

        wq, wk, wv = head_weights(w_query), head_weights(w_key), head_weights(w_value)
        bq = b_query.astype(F32).reshape(num_layers, 1, n)
        bk = b_key.astype(F32).reshape(num_layers, n, 1)
        bv = b_value.astype(F32).reshape(num_layers, n, 1)

        def permute(v, perm):
            return lax.ppermute(v, 'tp', perm)

        def gather_rel(own):
            two = jnp.concatenate([own, permute(own, FLIP_S)], axis=0)
            four = jnp.concatenate([two, permute(two, FLIP_F)], axis=0)
            return four, permute(four, FLIP_C)

        def ordered(bit, own, other):
            return jnp.where(bit == 0, jnp.concatenate([own, other], axis=0), jnp.concatenate([other, own], axis=0))

        def gather_rows(own):
            two = ordered(second, own, permute(own, FLIP_S))
            four = ordered(first, two, permute(two, FLIP_F))
            return ordered(core, four, permute(four, FLIP_C))

        def reduce_rows(send, keep, mid, bias):
            r = send.shape[0]

            def part(v, f, s=None):
                if s is None:
                    return lax.dynamic_slice(v, (f * (r // 2), 0), (r // 2, d)).astype(F32)
                return lax.dynamic_slice(v, (f * (r // 2) + s * (r // 4), 0), (r // 4, d)).astype(F32)

            def quarter(v, s):
                return lax.dynamic_slice(v, (s * (r // 4), 0), (r // 4, d)).astype(F32)

            got = permute(send, FLIP_C)
            out_f = (part(keep, 1 - first) + part(got, 1 - first)).astype(BF16)
            got_f = permute(out_f, FLIP_F)
            out_s = (part(keep, first, 1 - second) + part(got, first, 1 - second) + quarter(got_f, 1 - second)).astype(BF16)
            got_s = permute(out_s, FLIP_S)
            total = part(keep, first, second) + part(got, first, second) + quarter(got_f, second) + got_s.astype(F32)
            mine = lax.dynamic_slice(mid, ((core * 4 + first * 2 + second) * (r // 4), 0), (r // 4, d)).astype(F32)
            return (mine + total + bias.astype(F32)).astype(BF16)

        w_all = []
        for layer in range(num_layers):
            four, other = gather_rel(w_out[layer].reshape(1, n, d))
            w_all.append((four.reshape(4 * n, d), other.reshape(4 * n, d)))

        caches = None
        for layer in range(num_layers):
            g1, s1, g2, s2 = (v[layer][None].astype(F32) for v in (ln1_gain, ln1_bias, ln2_gain, ln2_bias))
            qs, ks, vs, ctx = {}, {}, {}, {}
            new = {}
            for c in 'PABC':
                which = jnp.stack([a_id if c in 'PA' else 1 - a_id]).astype(jnp.int32)
                qs[c], ks[c], vs[c], *caches = qkv(which, int(c in 'AC'), caches, (num_layers, prompts, n, 2 * seq_len), xs[c], g1, s1, wq, wk, wv, bq[layer], bk[layer], bv[layer], layer, scale)
                if c == 'P':
                    gathered = None
                else:
                    if c == 'A':
                        own = attend(zero, qs[c], [ks[c]], [vs[c]], heads)
                    elif c == 'B':
                        own = attend(pre_b1, qs[c], [ks[c]], [vs[c]], heads)
                    else:
                        own = attend(pre_b1, qs[c], [ks['B'], ks[c]], [vs['B'], vs[c]], heads)
                    gathered = gather_rel(own[None])
                send, keep, mid = mlp(core, gathered, w_all[layer], xs[c], b_out[layer][None].astype(F32), g2, s2, b_fc1[layer][None].astype(F32), w_fc1, w_fc2, layer)
                new[c] = gather_rows(reduce_rows(send, keep, mid, b_fc2[layer][None]))
            xs = new

        parts = list(lax.optimization_barrier(tuple(xs[c] for c in 'PABC')))
        out = jnp.where(swap, jnp.concatenate(parts[2:] + parts[:2], axis=0), jnp.concatenate(parts, axis=0)).reshape(prompts, seq_len, d)

        def cache(v):
            return jnp.transpose(v.reshape(num_layers, prompts, heads, head_dim, 2 * seq_len), (0, 1, 2, 4, 3))

        caches = zero_tail(caches)
        return out, cache(caches[0]), cache(caches[1])

    return jax.shard_map(local_run, mesh=mesh, in_specs=in_specs, out_specs=out_specs, check_vma=False)
```

```python
import functools

import jax
import jax.numpy as jnp
from jax import lax
from jax.experimental import pallas as pl
from jax.experimental.pallas import tpu as pltpu
from jax.sharding import PartitionSpec as P

LN_EPS = 1e-5
NT = (((1,), (1,)), ((), ()))
BLK = 256
F32 = jnp.float32
BF16 = jnp.bfloat16


FLIP_C = [(i, i ^ 1) for i in range(8)]
FLIP_F = [(i, i ^ (2 if i & 1 else 4)) for i in range(8)]
FLIP_S = [(i, i ^ (4 if i & 1 else 2)) for i in range(8)]


ORDER = 'MP0 QA0 TA0 QB0 TB0 QC0 TC0 QP0 MA0 MB0 MC0 QP1 MP1 QA1 TA1 QB1 TB1 QC1 TC1 MA1 MB1 MC1'


def norm_rows(x, gain, shift):
    center = x - jnp.mean(x, axis=-1, keepdims=True)
    variance = jnp.mean(center * center, axis=-1, keepdims=True)
    normed = center * lax.rsqrt(variance + LN_EPS)
    return (normed * gain + shift).astype(BF16)


def const_spec(shape, index):
    return pl.BlockSpec(shape, lambda *_: index, pipeline_mode=pl.Buffered(1))


def source_specs(src, rows, row_of):
    if src[0] == 'full':
        _, array, half = src
        d = array.shape[2]
        return [pl.BlockSpec((1, BLK, d), lambda i, m: (m[0], half * (rows // BLK) + row_of(i, m), 0))], [array]
    _, own, other = src
    d = own.shape[2]
    n = rows // BLK

    def piece(mine, sub):
        def index(i, m):
            block = row_of(i, m)
            first, second = (m[2], m[3]) if mine else (m[3], m[2])
            base = m[1] * (n // 2) if mine else (1 - m[1]) * (n // 2)
            local = jnp.clip(block - base, 0, n // 2 - 1)
            small = local * 2 + sub
            return (lax.bitwise_xor(small // 2, first) * 2 + lax.bitwise_xor(lax.rem(small, 2), second), 0, 0)
        return pl.BlockSpec((1, BLK // 2, d), index)

    return [piece(True, 0), piece(True, 1), piece(False, 0), piece(False, 1)], [own, own, other, other]


def source_block(refs, is_mine):
    if len(refs) == 1:
        return refs[0][0]
    return jnp.concatenate([jnp.where(is_mine, refs[0][0], refs[2][0]), jnp.where(is_mine, refs[1][0], refs[3][0])], axis=0)


ANY = pl.BlockSpec(memory_space=pl.ANY)


def qkv_kernel(scale, num_x, meta_ref, *refs):
    x_refs, refs = refs[:num_x], refs[num_x:]
    g_ref, s_ref, wq_ref, wk_ref, wv_ref, bq_ref, bk_ref, bv_ref = refs[:8]
    q_ref, k_ref, v_ref, kc_ref, vc_ref = refs[-5:]
    is_mine = pl.program_id(0) // (pl.num_programs(0) // 2) == meta_ref[1]
    h = norm_rows(source_block(x_refs, is_mine).astype(F32), g_ref[...], s_ref[...])
    q = lax.dot_general(h, wq_ref[0], NT, preferred_element_type=F32)
    q_ref[...] = ((q + bq_ref[...]) * scale).astype(BF16)
    k = (lax.dot_general(wk_ref[0], h, NT, preferred_element_type=F32) + bk_ref[...]).astype(BF16)
    v = (lax.dot_general(wv_ref[0], h, NT, preferred_element_type=F32) + bv_ref[...]).astype(BF16)
    k_ref[...] = k
    v_ref[...] = v
    kc_ref[0, 0] = k
    vc_ref[0, 0] = v


def qkv(meta, half, caches, cache_shape, src, rows, gain, shift, wq, wk, wv, bq, bk, bv, layer, scale, token):
    n, d = wq.shape[1:]
    blocks = rows // BLK
    w_spec = const_spec((1, n, d), (layer, 0, 0))
    x_specs, x_args = source_specs(src, rows, lambda i, m: i)
    in_specs = x_specs + [const_spec((1, d), (0, 0)), const_spec((1, d), (0, 0)),
                          w_spec, w_spec, w_spec, const_spec((1, n), (0, 0)), const_spec((n, 1), (0, 0)), const_spec((n, 1), (0, 0))]
    args = x_args + [gain, shift, wq, wk, wv, bq, bk, bv]
    aliases = {}
    if caches is not None:
        aliases = {len(args) + 1: 3, len(args) + 2: 4}
        in_specs += [ANY] * 2
        args += list(caches)
    in_specs += [ANY] * len(token)
    args += list(token)
    cache_spec = pl.BlockSpec((1, 1, n, BLK), lambda i, m: (layer, m[0], 0, half * blocks + i))
    return pl.pallas_call(
        functools.partial(qkv_kernel, scale, len(x_args)),
        grid_spec=pltpu.PrefetchScalarGridSpec(
            num_scalar_prefetch=1,
            grid=(blocks,),
            in_specs=in_specs,
            out_specs=[pl.BlockSpec((BLK, n), lambda i, m: (i, 0))] + [pl.BlockSpec((n, BLK), lambda i, m: (0, i))] * 2 + [cache_spec] * 2,
        ),
        out_shape=[jax.ShapeDtypeStruct((rows, n), BF16)] + [jax.ShapeDtypeStruct((n, rows), BF16)] * 2 + [jax.ShapeDtypeStruct(cache_shape, BF16)] * 2,
        input_output_aliases=aliases,
        cost_estimate=pl.CostEstimate(flops=6 * rows * d * 3 * n, bytes_accessed=rows * d * 2 + 3 * n * d * 2, transcendentals=0),
        name="ln_qkv",
    )(meta, *args)


def place_kernel(meta_ref, *refs):
    is_mine = pl.program_id(0) // (pl.num_programs(0) // 2) == meta_ref[1]
    refs[-1][0] = source_block(refs[:4], is_mine)


def place(meta, half, out, shape, src, rows):
    specs, args = source_specs(src, rows, lambda i, m: i)
    blocks = rows // BLK
    aliases = {}
    if out is not None:
        aliases = {len(args) + 1: 0}
        specs, args = specs + [ANY], args + [out]
    return pl.pallas_call(
        place_kernel,
        grid_spec=pltpu.PrefetchScalarGridSpec(
            num_scalar_prefetch=1,
            grid=(blocks,),
            in_specs=specs,
            out_specs=pl.BlockSpec((1, BLK, shape[2]), lambda i, m: (m[0], half * blocks + i, 0)),
        ),
        out_shape=jax.ShapeDtypeStruct(shape, BF16),
        input_output_aliases=aliases,
        cost_estimate=pl.CostEstimate(flops=rows * shape[2] * 1000, bytes_accessed=rows * shape[2] * 4, transcendentals=0),
        name="place",
    )(meta, *args)


def tail_kernel(kin, vin, kc_ref, vc_ref):
    kc_ref[...] = jnp.zeros_like(kc_ref)
    vc_ref[...] = jnp.zeros_like(vc_ref)


def zero_tail(caches):
    layers, prompts, n, length = caches[0].shape
    spec = pl.BlockSpec((1, 1, n, length // 2), lambda i, j: (i, j, 0, 1))
    return pl.pallas_call(
        tail_kernel,
        grid=(layers, prompts),
        in_specs=[pl.BlockSpec(memory_space=pl.ANY)] * 2,
        out_specs=[spec, spec],
        out_shape=[jax.ShapeDtypeStruct(v.shape, v.dtype) for v in caches],
        input_output_aliases={0: 0, 1: 1},
        name="zero_tail",
    )(*caches)


def attn_kernel(num_old, head_dim, *refs):
    prefix_ref, q_ref = refs[:2]
    k_refs = refs[2:2 + num_old + 1]
    v_refs = refs[2 + num_old + 1:4 + 2 * num_old]
    c_ref = refs[-1]
    head = pl.program_id(0)
    rows, n = q_ref.shape
    lane = lax.broadcasted_iota(jnp.int32, (1, n), 1)
    mine = lane // head_dim == head
    prefix = prefix_ref[0]
    diag = lax.broadcasted_iota(jnp.int32, (BLK, BLK), 1) <= lax.broadcasted_iota(jnp.int32, (BLK, BLK), 0)
    for i in range(rows // BLK):
        q = jnp.where(mine, q_ref[pl.ds(i * BLK, BLK), :], 0)
        pieces = []
        base = 0
        for k_ref, v_ref in zip(k_refs, v_refs):
            last = base == num_old * rows
            size = (i + 1) * BLK if last else rows
            for lo in range(0, size, BLK):
                width = BLK
                s = jnp.dot(q, k_ref[:, pl.ds(lo, width)], preferred_element_type=F32)
                if base == 0:
                    key = lax.broadcasted_iota(jnp.int32, (1, width), 1) + lo
                    s = s + jnp.where(key >= prefix, 0.0, -jnp.inf)
                if last and lo == i * BLK:
                    s = jnp.where(diag, s, -jnp.inf)
                pieces.append((s, v_ref, lo))
            base += rows
        top = pieces[0][0]
        for s, _, _ in pieces[1:]:
            top = jnp.maximum(top, s)
        row_max = jnp.maximum(jnp.max(top, axis=-1, keepdims=True), -1e30)
        total = None
        ctx = None
        for s, v_ref, lo in pieces:
            p = jnp.exp(s - row_max)
            total = p if total is None else total + p
            part = lax.dot_general(p.astype(BF16), v_ref[:, pl.ds(lo, BLK)], NT, preferred_element_type=F32)
            ctx = part if ctx is None else ctx + part
        row_sum = jnp.sum(total, axis=-1, keepdims=True)
        out = (ctx / jnp.maximum(row_sum, 1.0)).astype(BF16)
        here = pl.ds(i * BLK, BLK)
        c_ref[here, :] = jnp.where(mine, out, c_ref[here, :])


def attend(prefix, q, ks, vs, heads, token):
    rows, n = q.shape
    num_old = len(ks) - 1
    whole = [const_spec(q.shape, (0, 0))] + [const_spec(k.shape, (0, 0)) for k in ks] * 2
    area = rows * rows * num_old + rows * rows // 2
    return pl.pallas_call(
        functools.partial(attn_kernel, num_old, n // heads),
        grid=(heads,),
        in_specs=[pl.BlockSpec(memory_space=pltpu.SMEM)] + whole + [ANY] * len(token),
        out_specs=pl.BlockSpec((rows, n), lambda i: (0, 0)),
        out_shape=jax.ShapeDtypeStruct((rows, n), BF16),
        cost_estimate=pl.CostEstimate(flops=area * heads * n * 8, bytes_accessed=rows * n * 8, transcendentals=area * heads),
        name="attend",
    )(prefix, q, *ks, *vs, *token)


def mlp_kernel(with_attn, num_x, meta_ref, *refs):
    if with_attn:
        c_lo, c_hi, w_lo, w_hi = refs[:4]
        refs = refs[4:]
        c_all = refs[-1]
        refs = refs[:-1]
    x_refs, refs = refs[:num_x], refs[num_x:]
    bo_ref, g_ref, s_ref, b1_ref, w1_ref, w2_ref = refs[:6]
    send_ref, keep_ref, mid_ref = refs[-3:]
    i = pl.program_id(0)
    half = pl.num_programs(0) // 2
    x = source_block(x_refs, i >= half).astype(F32)
    if with_attn:
        for j in range(4):
            c_all[0, :, j * 256:(j + 1) * 256] = c_lo[j]
            c_all[1, :, j * 256:(j + 1) * 256] = c_hi[j]
        attn = jnp.dot(c_all[0], w_lo[...], preferred_element_type=F32) + jnp.dot(c_all[1], w_hi[...], preferred_element_type=F32)
        x = x + attn
    mid = (x + bo_ref[...]).astype(BF16)
    mid_ref[...] = mid
    g = norm_rows(mid.astype(F32), g_ref[...], s_ref[...])
    u = jnp.dot(g, w1_ref[0], preferred_element_type=F32) + b1_ref[...]
    u = jnp.maximum(u, 0.0).astype(BF16)
    part = jnp.dot(u, w2_ref[0], preferred_element_type=F32).astype(BF16)

    @pl.when(i < half)
    def _():
        send_ref[...] = part

    @pl.when(i >= half)
    def _():
        keep_ref[...] = part


def mlp(meta, ctx, w_out, src, rows, b_out, gain, shift, b1, w1, w2, layer, token):
    d, f = w1.shape[1:]
    n = rows // BLK
    half = n // 2
    row_of = lambda i, m: lax.rem(i + (1 - m[1]) * half, n)
    in_specs, args, scratch = [], [], []
    if ctx is not None:
        in_specs += [pl.BlockSpec((4, BLK, 256), lambda i, m: (0, row_of(i, m), 0))] * 2
        in_specs += [const_spec((d // 2, d), (0, 0))] * 2
        args += [*ctx, *w_out]
        scratch = [pltpu.VMEM((2, BLK, d // 2), BF16)]
    x_specs, x_args = source_specs(src, rows, row_of)
    in_specs += x_specs + [const_spec((1, d), (0, 0))] * 3
    in_specs += [const_spec((1, f), (0, 0)), const_spec((1, d, f), (layer, 0, 0)), const_spec((1, f, d), (layer, 0, 0))]
    args += x_args + [b_out, gain, shift, b1, w1, w2]
    in_specs += [ANY] * len(token)
    args += list(token)
    flops = 4 * rows * d * f + (2 * rows * d * d if ctx is not None else 0)
    return pl.pallas_call(
        functools.partial(mlp_kernel, ctx is not None, len(x_args)),
        grid_spec=pltpu.PrefetchScalarGridSpec(
            num_scalar_prefetch=1,
            grid=(n,),
            in_specs=in_specs,
            out_specs=[pl.BlockSpec((BLK, d), lambda i, m: (jnp.minimum(i, half - 1), 0)),
                       pl.BlockSpec((BLK, d), lambda i, m: (jnp.maximum(i - half, 0), 0)),
                       pl.BlockSpec((BLK, d), lambda i, m: (row_of(i, m), 0))],
            scratch_shapes=scratch,
        ),
        out_shape=[jax.ShapeDtypeStruct((rows // 2, d), BF16), jax.ShapeDtypeStruct((rows // 2, d), BF16), jax.ShapeDtypeStruct((rows, d), BF16)],
        compiler_params=pltpu.CompilerParams(vmem_limit_bytes=56 * 1024 * 1024),
        cost_estimate=pl.CostEstimate(flops=3 * flops, bytes_accessed=rows * d * 8 + 4 * d * f, transcendentals=0),
        name="proj_mlp" if ctx is not None else "mlp",
    )(meta, *args)


def solution(mesh):
    rep_vec = P(None, None)
    head_w = P(None, None, 'tp', None)
    head_b = P(None, 'tp', None)
    out_w = P(None, 'tp', None, None)
    in_specs = (P('dp', None, None), P('dp', None), rep_vec, rep_vec, head_w, head_b, head_w, head_b, head_w, head_b,
                out_w, rep_vec, rep_vec, rep_vec, P(None, None, 'tp'), P(None, 'tp'), P(None, 'tp', None), rep_vec)
    cache_spec = P(None, 'dp', 'tp', None, None)
    out_specs = (P('dp', None, None), cache_spec, cache_spec)

    def local_run(hidden, attn_mask, ln1_gain, ln1_bias, w_query, b_query, w_key, b_key, w_value, b_value, w_out, b_out, ln2_gain, ln2_bias, w_fc1, b_fc1, w_fc2, b_fc2):
        prompts, seq_len, d = hidden.shape
        num_layers, _, heads, head_dim = w_query.shape
        n = heads * head_dim
        rows = seq_len // 2
        scale = head_dim ** -0.5
        me = lax.axis_index('tp')
        core = me % 2
        bit_x, bit_y = (me // 2) % 2, me // 4
        first = jnp.where(core == 0, bit_y, bit_x)
        second = jnp.where(core == 0, bit_x, bit_y)

        prefix = jnp.sum((attn_mask == 0).astype(jnp.int32), axis=1)
        swap = prefix[1] == rows
        pre_a = jnp.where(swap, prefix[1], prefix[0])
        pre_b = jnp.where(swap, prefix[0], prefix[1])
        zero = jnp.zeros((1,), jnp.int32)
        pre_b1 = jnp.stack([pre_b])
        a_id = jnp.where(swap, 1, 0)
        metas = {c: jnp.stack([a_id if c in 'PA' else 1 - a_id, core, first, second]).astype(jnp.int32) for c in 'PABC'}
        half_of = {'P': 0, 'A': 1, 'B': 0, 'C': 1}
        xs = {c: ('full', hidden, half_of[c]) for c in 'PABC'}

        def head_weights(w):
            return jnp.transpose(w, (0, 2, 3, 1)).reshape(num_layers, n, d)

        wq, wk, wv = head_weights(w_query), head_weights(w_key), head_weights(w_value)
        bq = b_query.astype(F32).reshape(num_layers, 1, n)
        bk = b_key.astype(F32).reshape(num_layers, n, 1)
        bv = b_value.astype(F32).reshape(num_layers, n, 1)

        def permute(v, perm):
            return lax.ppermute(v, 'tp', perm)

        def gather_rel(own):
            two = jnp.concatenate([own, permute(own, FLIP_S)], axis=0)
            four = jnp.concatenate([two, permute(two, FLIP_F)], axis=0)
            return four, permute(four, FLIP_C)

        def reduce_rows(send, keep, mid, bias):
            r = send.shape[0]

            def part(v, f, s=None):
                if s is None:
                    return lax.dynamic_slice(v, (f * (r // 2), 0), (r // 2, d)).astype(F32)
                return lax.dynamic_slice(v, (f * (r // 2) + s * (r // 4), 0), (r // 4, d)).astype(F32)

            def quarter(v, s):
                return lax.dynamic_slice(v, (s * (r // 4), 0), (r // 4, d)).astype(F32)

            got = permute(send, FLIP_C)
            out_f = (part(keep, 1 - first) + part(got, 1 - first)).astype(BF16)
            got_f = permute(out_f, FLIP_F)
            out_s = (part(keep, first, 1 - second) + part(got, first, 1 - second) + quarter(got_f, 1 - second)).astype(BF16)
            got_s = permute(out_s, FLIP_S)
            total = part(keep, first, second) + part(got, first, second) + quarter(got_f, second) + got_s.astype(F32)
            mine = lax.dynamic_slice(mid, ((core * 4 + first * 2 + second) * (r // 4), 0), (r // 4, d)).astype(F32)
            return (mine + total + bias.astype(F32)).astype(BF16)

        w_all = []
        for layer in range(num_layers):
            four, other = gather_rel(w_out[layer].reshape(1, n, d))
            w_all.append((four.reshape(4 * n, d), other.reshape(4 * n, d)))

        caches = None
        cache_shape = (num_layers, prompts, n, 2 * seq_len)
        token = []
        vecs = [[v[layer][None].astype(F32) for v in (ln1_gain, ln1_bias, ln2_gain, ln2_bias, b_out, b_fc1)] for layer in range(num_layers)]
        state = {}
        sources = [xs, {}, {}]

        def run(step):
            nonlocal caches, token
            kind, c, layer = step[0], step[1], int(step[2])
            g1, s1, g2, s2, bo, b1 = vecs[layer]
            src = sources[layer][c]
            if kind == 'Q':
                q, k, v, *caches = qkv(metas[c], half_of[c], caches, cache_shape, src, rows, g1, s1, wq, wk, wv, bq[layer], bk[layer], bv[layer], layer, scale, token)
                state[c, layer] = q, k, v
                token = [q]
            if kind == 'T':
                q, k, v = state[c, layer]
                ks, vs = [k], [v]
                if c == 'C':
                    _, k, v = state['B', layer]
                    ks, vs = [k] + ks, [v] + vs
                own = attend(zero if c == 'A' else pre_b1, q, ks, vs, heads, token)
                state['ctx', c, layer] = gather_rel(own[None])
                token = [own]
            if kind == 'M':
                ctx = state.get(('ctx', c, layer))
                send, keep, mid = mlp(metas[c], ctx, w_all[layer], src, rows, bo, g2, s2, b1, w_fc1, w_fc2, layer, token)
                token = [send]
                own = reduce_rows(send, keep, mid, b_fc2[layer][None])
                sources[layer + 1][c] = ('pieces', *gather_rel(own[None]))

        for step in ORDER.split():
            run(step)

        out = None
        for c in 'PABC':
            out = place(metas[c], half_of[c], out, hidden.shape, sources[2][c], rows)

        def cache(v):
            return jnp.transpose(v.reshape(num_layers, prompts, heads, head_dim, 2 * seq_len), (0, 1, 2, 4, 3))

        caches = zero_tail(caches)
        return out, cache(caches[0]), cache(caches[1])

    return jax.shard_map(local_run, mesh=mesh, in_specs=in_specs, out_specs=out_specs, check_vma=False)
```
